32 devices in a mesh: dp: 8 (over y, x, core), fsdp: 4 (over z).
Axes of the slice: x: 2, y: 2, z: 4, core: 2. Of those that a mesh axis runs over, the one named last changes fastest.
Arguments:
- tokens: bfloat16 [4096, 4096], P('dp'), may hold values from -6 to 6
- counts: int32 [8], P('dp'), may hold values from 256 to 512, as said below
- patch_index: int32 [4096], P('dp'), may hold values from 0 to 255
- clip_limit: float32 [], replicated, may hold values from 1024 to 8192
- norm_gain: float32 [4, 4096], replicated, may hold values from 0.25 to 1.75
- params: float32 [4, 4096, 4096], P(None, 'dp', 'fsdp'), may hold values from -0.09375 to 0.09375
- moments: float32 [4, 4096, 4096], P(None, 'dp', 'fsdp'), may hold values from -0.3 to 0.3
- seconds: float32 [4, 4096, 4096], P(None, 'dp', 'fsdp'), may hold values from 0.05 to 1
- gradients: float32 [4, 4096, 4096], P(None, 'dp', 'fsdp'), may hold values from -48 to 48
Outputs:
- params_new: float32 [4, 4096, 4096], P(None, 'dp', 'fsdp')
- moments_new: float32 [4, 4096, 4096], P(None, 'dp', 'fsdp')
- seconds_new: float32 [4, 4096, 4096], P(None, 'dp', 'fsdp')
- mixed: bfloat16 [4096, 4096], P('dp', 'fsdp')
The draws below stay inside these ranges and needn't reach their ends.
Inputs may be any that keep to these rules, and one draw needn't show every extreme that they name: `counts`: at most 512, reached on some index of dp in every draw.
All inputs are finite; a program needn't handle non-finite values.
Results may differ from the reference program's by a relative error of at most 0.0095.
Values may be sent and summed in bfloat16 or wider, within the bound.
A program may use at most 192 MiB of HBM per device.

```python
import math
import jax
import jax.numpy as jnp
from jax import lax

D = 4096
TOK_DEV = 512
LAYERS = 4
GRID = 16
STEP = 40
TOKENS = 4096
N_DP = 8


def draw_counts(key, part):
    drawn = jax.random.randint(key, (N_DP,), TOK_DEV // 2, TOK_DEV + 1)
    chosen = jax.random.randint(jax.random.fold_in(key, 3), (), 0, N_DP)
    return jnp.where(jnp.arange(N_DP) == chosen, TOK_DEV, drawn).astype(jnp.int32)


def draw_gradients(key, part):
    rising = jnp.arange(D, dtype=jnp.float32)[None, :, None] / D
    scaling = 1.0 + 2.0 * rising
    noise = jnp.clip(jax.random.normal(key, (LAYERS, D, D), jnp.float32), -6.0, 6.0)
    return scaling * noise


def with_ends(values, key, low, high):
    longest = values.shape.index(max(values.shape))
    spots = []
    for shift in (0, 1):
        where = [jax.random.randint(jax.random.fold_in(key, axis), (), 0, length) for axis, length in enumerate(values.shape)]
        where[longest] = (where[longest] + shift) % values.shape[longest]
        spots.append(tuple(where))
    return values.at[spots[0]].set(low).at[spots[1]].set(high)


def block_scale(own_key, shape, cuts, smallest, high):
    factor_of = 1.0
    for dim, shards_of in cuts:
        draws = jax.random.uniform(jax.random.fold_in(jax.random.fold_in(own_key, 6), dim), (shards_of,), jnp.float32, smallest / len(cuts), high / len(cuts))
        factor_of = factor_of * jnp.repeat(jnp.exp(draws), shape[dim] // shards_of).reshape((-1,) + (1,) * (len(shape) - 1 - dim))
    return factor_of


def normal_values(key, dims, deviation, limit, split=(), held_as=jnp.bfloat16):
    entries = jax.random.normal(key, dims, jnp.float32) * deviation
    if len(split) > 0:
        entries = block_scale(key, dims, split, -0.22, 0.18) * entries
    return jnp.clip(entries, min=-limit, max=limit).astype(held_as)


def setup_inputs(seed: int = 0) -> dict:
    seeds = jax.random.split(jax.random.key(seed), 10)
    tokens = normal_values(seeds[0], (TOKENS, D), 1.0, 6.0, ((0, 8),))
    counts = draw_counts(jax.random.fold_in(seeds[9], 71), 0)
    patch_index = with_ends(jax.random.randint(seeds[2], (TOKENS,), 0, GRID * GRID), jax.random.fold_in(seeds[2], 1), 0, (GRID * GRID) - 1).astype(jnp.int32)
    clip_limit = jnp.clip(jnp.exp(jax.random.uniform(seeds[3], (), jnp.float32, math.log(1024.0), math.log(8192.0))), 1024.0, 8192.0)
    norm_gain = jnp.clip(1.0 + 0.15 * jax.random.normal(seeds[4], (LAYERS, D), jnp.float32), 0.25, 1.75)
    params = normal_values(seeds[5], (LAYERS, D, D), D ** -0.5, 0.09375, ((1, 8), (2, 4)), jnp.float32)
    moments = normal_values(seeds[6], (LAYERS, D, D), 0.05, 0.3, ((1, 8), (2, 4)), jnp.float32)
    seconds = jnp.clip(jnp.exp(math.log(1.0) - 2.9957323 * jax.random.uniform(seeds[7], (LAYERS, D, D), jnp.float32) ** block_scale(seeds[7], (LAYERS, D, D), ((1, 8), (2, 4)), -0.2, 0.2)), 0.05, 1.0)
    gradients = draw_gradients(jax.random.fold_in(seeds[9], 71), 0)
    return dict(tokens=tokens, counts=counts, patch_index=patch_index, clip_limit=clip_limit, norm_gain=norm_gain, params=params, moments=moments, seconds=seconds, gradients=gradients)


beta_one = 0.9
beta_two = 0.95
adam_eps = 1e-08
learning_rate = 0.0024
weight_decay = 0.05
norm_eps = 1e-06

def position_code(patch_index):
    quarter = D // 4
    freqs = 1.0 / 10000.0 ** (jnp.arange(quarter, dtype=jnp.float32) / quarter)
    across = (patch_index // GRID).astype(jnp.float32)[:, None] * freqs[None, :]
    downward = (patch_index % GRID).astype(jnp.float32)[:, None] * freqs[None, :]
    return jnp.concatenate([jnp.sin(across), jnp.cos(across), jnp.sin(downward), jnp.cos(downward)], axis=1)

def layer_norm(stream, gain_row):
    centre = lax.optimization_barrier(jnp.mean(stream, axis=1, keepdims=True))
    shifted = stream - centre
    spread = lax.optimization_barrier(jnp.mean(shifted * shifted, axis=1, keepdims=True))
    return (shifted * lax.rsqrt(spread + norm_eps) * gain_row[None, :]).astype(jnp.bfloat16)

def adam_update(params, moments, seconds, gradients, factor):
    clipped = gradients * factor
    moments_new = beta_one * moments + (1.0 - beta_one) * clipped
    seconds_new = beta_two * seconds + (1.0 - beta_two) * clipped * clipped
    direction = moments_new / (1.0 - beta_one ** STEP) / (jnp.sqrt(seconds_new / (1.0 - beta_two ** STEP)) + adam_eps)
    params_new = params - learning_rate * (direction + weight_decay * params)
    return (params_new, moments_new, seconds_new)

def reference(tokens, counts, patch_index, clip_limit, norm_gain, params, moments, seconds, gradients):
    squares = jnp.sum(gradients * gradients)
    factor = jnp.minimum(1.0, clip_limit / (jnp.sqrt(squares) + 1e-06))
    params_new, moments_new, seconds_new = adam_update(params, moments, seconds, gradients, factor)
    weights = params_new.astype(jnp.bfloat16)
    slot = jnp.arange(TOKENS, dtype=jnp.int32) % TOK_DEV
    valid = (slot < jnp.repeat(counts, TOK_DEV, total_repeat_length=TOKENS))[:, None]
    stream = jnp.where(valid, tokens.astype(jnp.float32) + position_code(patch_index), 0.0)
    for current in range(LAYERS):
        normed = layer_norm(stream, norm_gain[current])
        branch = jnp.dot(normed, weights[current], preferred_element_type=jnp.float32).astype(jnp.bfloat16)
        stream = stream + branch.astype(jnp.float32)
    mixed = jnp.where(valid, stream, 0.0).astype(jnp.bfloat16)
    return (params_new, moments_new, seconds_new, mixed)
```

```python
import functools
import jax
import jax.numpy as jnp
from jax import lax
from jax.experimental import pallas as pl
from jax.experimental.pallas import tpu as pltpu
from jax.sharding import PartitionSpec as P

GRID = 16
STEP = 40

beta_one = 0.9
beta_two = 0.95
adam_eps = 1e-08
learning_rate = 0.0024
weight_decay = 0.05
norm_eps = 1e-06

MESH = pl.DeviceIdType.MESH
ANY = pl.BlockSpec(memory_space=pl.ANY)
VMEM = pl.BlockSpec(memory_space=pltpu.VMEM)
SMEM = pl.BlockSpec(memory_space=pltpu.SMEM)


def adam_update(params, moments, seconds, gradients, factor):
    clipped = gradients * factor
    moments_new = beta_one * moments + (1.0 - beta_one) * clipped
    seconds_new = beta_two * seconds + (1.0 - beta_two) * clipped * clipped
    direction = (moments_new * (1.0 / (1.0 - beta_one**STEP))) / (
        jnp.sqrt(seconds_new * (1.0 / (1.0 - beta_two**STEP))) + adam_eps
    )
    params_new = params - learning_rate * (direction + weight_decay * params)
    return (params_new, moments_new, seconds_new)


def total_kernel(sizes, chunks, clip_ref, g_ref, p_ref, m_ref, s_ref, factor_ref, head_ref, *scratch):
    g, p, m, s, mine, mid, got0, got1 = scratch[:8]
    g_sem, a_sem, send0, send1, recv0, recv1 = scratch[8:]
    names, got, send, recv = ("dp", "fsdp"), (got0, got1), (send0, send1), (recv0, recv1)
    place = [lax.axis_index(name) for name in names]
    layers, rows, cols = g.shape
    part = rows // chunks

    def take_gradients(l, c):
        at = pl.ds(pl.multiple_of(c * part, part), part)
        return pltpu.make_async_copy(g_ref.at[l, at], g.at[l, at], g_sem.at[l, c])

    def start_layer(l, carry):
        lax.fori_loop(0, chunks, lambda c, x: (take_gradients(l, c).start(), x)[1], 0)
        return carry

    lax.fori_loop(0, layers, start_layer, 0)
    heads = [
        pltpu.make_async_copy(ref.at[0], to, a_sem.at[i])
        for i, (ref, to) in enumerate(((p_ref, p), (m_ref, m), (s_ref, s)))
    ]
    for copy in heads:
        copy.start()
    barrier = pltpu.get_barrier_semaphore()
    for axis in range(2):
        for step in range(1, sizes[axis]):
            pl.semaphore_signal(
                barrier,
                inc=1,
                device_id={names[axis]: lax.rem(place[axis] + step, sizes[axis])},
                device_id_type=MESH,
            )

    def add_layer(l, total):
        def add_chunk(c, total):
            take_gradients(l, c).wait()

            def add_rows(k, total):
                x = g[l, pl.ds(pl.multiple_of(c * part + k * 32, 32), 32)]
                x = x * x
                sums = [x[8 * i : 8 * i + 8] for i in range(4)]
                y = (sums[0] + sums[1]) + (sums[2] + sums[3])
                return total + y

            return lax.fori_loop(0, part // 32, add_rows, total)

        return lax.fori_loop(0, chunks, add_chunk, total)

    wide = lax.fori_loop(0, layers, add_layer, jnp.zeros((8, cols), jnp.float32))
    total = wide[:, 0:128]
    for k in range(1, cols // 128):
        total = total + wide[:, 128 * k : 128 * k + 128]
    mine[...] = total

    pl.semaphore_wait(barrier, sizes[0] + sizes[1] - 2)
    for axis in range(2):
        source = mine if axis == 0 else mid
        copies = []
        for step in range(1, sizes[axis]):
            copy = pltpu.make_async_remote_copy(
                src_ref=source,
                dst_ref=got[axis].at[place[axis]],
                send_sem=send[axis].at[step - 1],
                recv_sem=recv[axis].at[step - 1],
                device_id={names[axis]: lax.rem(place[axis] + step, sizes[axis])},
                device_id_type=MESH,
            )
            copy.start()
            copies.append(copy)
        got[axis][place[axis]] = source[...]
        for copy in copies:
            copy.wait()
        total = got[axis][0]
        for slot in range(1, sizes[axis]):
            total = total + got[axis][slot]
        if axis == 0:
            mid[...] = total
    squares = jnp.sum(jnp.sum(total, axis=1, keepdims=True), axis=0, keepdims=True)
    factor = jnp.minimum(1.0, clip_ref[0] / (jnp.sqrt(squares) + 1e-06))
    factor_ref[...] = jnp.broadcast_to(factor, factor_ref.shape)
    for copy in heads:
        copy.wait()

    def update(k, carry):
        at = pl.ds(pl.multiple_of(k * 16, 16), 16)
        head_ref[at] = adam_update(p[at], m[at], s[at], g[0, at], factor)[0].astype(jnp.bfloat16)
        return carry

    lax.fori_loop(0, rows // 16, update, 0)


def total_over_mesh(sizes, clip_limit, gradients, params, moments, seconds):
    layers, rows, cols = gradients.shape
    shape, f32, dma = (8, 128), jnp.float32, pltpu.SemaphoreType.DMA
    chunks = 2
    return pl.pallas_call(
        functools.partial(total_kernel, sizes, chunks),
        out_shape=[
            jax.ShapeDtypeStruct((8, 128), f32),
            jax.ShapeDtypeStruct((rows, cols), jnp.bfloat16),
        ],
        in_specs=[SMEM, ANY, ANY, ANY, ANY],
        out_specs=[VMEM, VMEM],
        scratch_shapes=[pltpu.VMEM((layers, rows, cols), f32)]
        + [pltpu.VMEM((rows, cols), f32)] * 3
        + [pltpu.VMEM(shape, f32)] * 2
        + [pltpu.VMEM((size,) + shape, f32) for size in sizes]
        + [dma((layers, chunks)), dma((3,))]
        + [dma((max(size - 1, 1),)) for size in sizes] * 2,
        compiler_params=pltpu.CompilerParams(
            collective_id=0, has_side_effects=True, vmem_limit_bytes=63 * 2**20
        ),
        name="total",
    )(clip_limit[None], gradients, params, moments, seconds)


def adam_kernel(f_ref, p_ref, m_ref, s_ref, g_ref, po_ref, mo_ref, so_ref, w_ref):
    factor = f_ref[0:1, 0:1]

    def update(k, carry):
        at = pl.ds(pl.multiple_of(k * 16, 16), 16)
        new = adam_update(p_ref[0, at], m_ref[0, at], s_ref[0, at], g_ref[0, at], factor)
        po_ref[0, at], mo_ref[0, at], so_ref[0, at] = new
        w_ref[0, at] = new[0].astype(jnp.bfloat16)
        return carry

    lax.fori_loop(0, p_ref.shape[1] // 16, update, 0)


def adam_all(factor, params, moments, seconds, gradients):
    layers, rows, cols = params.shape
    part = 128
    block = pl.BlockSpec((1, part, cols), lambda l, c: (l, c, 0))
    f32 = jax.ShapeDtypeStruct(params.shape, jnp.float32)
    return pl.pallas_call(
        adam_kernel,
        grid=(layers, rows // part),
        out_shape=[f32, f32, f32, jax.ShapeDtypeStruct(params.shape, jnp.bfloat16)],
        in_specs=[pl.BlockSpec((8, 128), lambda l, c: (0, 0))] + [block] * 4,
        out_specs=[block] * 4,
        compiler_params=pltpu.CompilerParams(vmem_limit_bytes=63 * 2**20),
        cost_estimate=pl.CostEstimate(
            flops=20 * params.size, bytes_accessed=30 * params.size, transcendentals=0
        ),
        name="adam",
    )(factor, params, moments, seconds, gradients)


def layers_kernel(n_dp, n, chunks, names, *refs):
    r = dict(zip(names, refs))
    layers, rows, cols = r["own"].shape
    tok, width = r["stream"].shape
    part = tok // chunks
    tile = min(256, cols)
    tiles = cols // tile
    sub_rows = rows // 2
    ring = n_dp // 2
    half = ring // 2
    hops = n - 1
    dp, place = lax.axis_index("dp"), lax.axis_index("fsdp")
    chip, core = dp // 2, lax.rem(dp, 2)
    count = r["counts"][0]

    def turn(i):
        if ring != 4:
            return i
        return (i // 2) * 2 + lax.rem(i + i // 2, 2)

    pos = turn(chip)

    def dp_of(position, which):
        return turn(lax.rem(position + 2 * ring, ring)) * 2 + which

    def w_rows(position, which, sub):
        at = dp_of(position, which) * rows + sub * sub_rows
        return pl.ds(pl.multiple_of(at, sub_rows), sub_rows)

    def rows_of(c):
        return pl.ds(pl.multiple_of(c * part, part), part)

    def cols_of(owner):
        return pl.ds(pl.multiple_of(owner * cols, cols), cols)

    def take_own(l):
        return pltpu.make_async_copy(
            r["own"].at[l],
            r["w"].at[l, pl.ds(pl.multiple_of(dp * rows, rows), rows)],
            r["own_sem"].at[l],
        )

    def ring_copy(l, way, hop, sub):
        owner = pos - hop if way == 0 else pos + hop
        at = w_rows(owner, core, sub)
        return pltpu.make_async_remote_copy(
            src_ref=r["w"].at[l, at],
            dst_ref=r["w"].at[l, at],
            send_sem=r["ring_send"].at[l, way, hop, sub],
            recv_sem=r["ring_recv"].at[l, way, hop, sub],
            device_id={"dp": dp_of(pos + 1 if way == 0 else pos - 1, core)},
            device_id_type=MESH,
        )

    def mate_copy(l, owner, slot, sub):
        at = w_rows(owner, core, sub)
        return pltpu.make_async_remote_copy(
            src_ref=r["w"].at[l, at],
            dst_ref=r["w"].at[l, at],
            send_sem=r["mate_send"].at[l, slot, sub],
            recv_sem=r["mate_recv"].at[l, slot, sub],
            device_id={"dp": chip * 2 + 1 - core},
            device_id_type=MESH,
        )

    def came(way, hop):
        return pos - 1 - hop if way == 0 else pos + 1 + hop

    def all_mates():
        out = [(pos, 0, 0), (pos, 0, 1)]
        for hop in range(half):
            for way in range(2):
                for sub in range(2):
                    if hop < half - 1 or sub == way:
                        out.append((came(way, hop), 1 + 2 * hop + way, sub))
        return out

    def all_rings():
        out = []
        for hop in range(half):
            for way in range(2):
                for sub in range(2):
                    if hop < half - 1 or sub == way:
                        out.append((way, hop, sub))
        return out

    ring_order = ((0, 0), (1, 1), (0, 1), (1, 0))

    def gather_start(l):
        take_own(l).wait()
        for way, sub in ring_order:
            if half > 1 or sub == way:
                ring_copy(l, way, 0, sub).start()
        for sub in range(2):
            mate_copy(l, pos, 0, sub).start()

    def gather_mid(l):
        for hop in range(half - 1):
            for way, sub in ring_order:
                ring_copy(l, way, hop, sub).wait_recv()
                if hop + 1 < half - 1 or sub == way:
                    ring_copy(l, way, hop + 1, sub).start()
                mate_copy(l, came(way, hop), 1 + 2 * hop + way, sub).start()

    def gather_end(l):
        hop = half - 1
        for way in range(2):
            ring_copy(l, way, hop, way).wait_recv()
            mate_copy(l, came(way, hop), 1 + 2 * hop + way, way).start()
        for owner, slot, sub in all_mates():
            mate_copy(l, owner, slot, sub).wait_recv()

    def pass_on(l, way, hop, c):
        owner = place - hop if way == 0 else place + hop
        peer = lax.rem(place + 1, n) if way == 0 else lax.rem(place + n - 1, n)
        target = r["b"].at[l, rows_of(c), cols_of(owner)]
        return pltpu.make_async_remote_copy(
            src_ref=target,
            dst_ref=target,
            send_sem=r["send"].at[l, way, hop, c],
            recv_sem=r["recv"].at[l, way, hop, c],
            device_id={"fsdp": peer},
            device_id_type=MESH,
        )

    def has_sent(way, hop):
        if way == 0:
            return jnp.logical_and(place < n - 1, place >= hop)
        return jnp.logical_and(place > 0, place + hop < n)

    def has_got(way, hop):
        return place >= hop + 1 if way == 0 else place + hop + 1 < n

    take_tokens = pltpu.make_async_copy(r["tokens"], r["b"].at[layers - 2], r["tok_sem"].at[0])
    take_tokens.start()
    for l in range(layers):
        take_own(l).start()

    barrier = pltpu.get_barrier_semaphore()
    peers = [{"fsdp": lax.rem(place + 1, n)}, {"fsdp": lax.rem(place + n - 1, n)}]
    peers += [{"dp": dp_of(pos + 1, core)}, {"dp": dp_of(pos - 1, core)}]
    peers += [{"dp": chip * 2 + 1 - core}]
    for peer in peers:
        pl.semaphore_signal(barrier, inc=1, device_id=peer, device_id_type=MESH)
    pl.semaphore_wait(barrier, len(peers))

    gather_start(0)
    take_tokens.wait()

    def init_body(t, carry):
        at = pl.ds(pl.multiple_of(t * tile, tile), tile)
        code = jnp.dot(r["hot"][...], r["table"][:, at], preferred_element_type=jnp.float32)
        slot = lax.broadcasted_iota(jnp.int32, code.shape, 0)
        value = r["b"][layers - 2, :, at].astype(jnp.float32) + code
        r["stream"][:, at] = jnp.where(slot < count, value, 0.0)
        return carry

    lax.fori_loop(0, width // tile, init_body, 0)
    gather_mid(0)
    gather_end(0)

    sub = 32

    def norm_chunk(l, c):
        def norm_body(k, carry):
            at = pl.ds(pl.multiple_of(c * part + k * sub, sub), sub)
            x = r["stream"][at]
            centre = jnp.sum(x, axis=1, keepdims=True) * (1.0 / width)
            shifted = x - centre
            spread = jnp.sum(shifted * shifted, axis=1, keepdims=True) * (1.0 / width)
            normed = shifted * lax.rsqrt(spread + norm_eps) * r["gain"][l]
            r["x"][pl.ds(pl.multiple_of(k * sub, sub), sub)] = normed.astype(jnp.bfloat16)
            return carry

        lax.fori_loop(0, part // sub, norm_body, 0)

    def add_chunk(l, c):
        for way in range(2):

            @pl.when(has_got(way, hops - 1))
            def _():
                pass_on(l - 1, way, hops - 1, c).wait_recv()

        def add_body(k, carry):
            at = pl.ds(pl.multiple_of(c * part + k * sub, sub), sub)
            r["stream"][at] = r["stream"][at] + r["b"][l - 1, at].astype(jnp.float32)
            return carry

        lax.fori_loop(0, part // sub, add_body, 0)

    def layer_body(l, carry):
        gather_start(l + 1)

        def chunk_body(c, carry):
            @pl.when(l > 0)
            def _():
                add_chunk(l, c)

            norm_chunk(l, c)

            def dot_body(t, carry):
                at = pl.ds(pl.multiple_of(t * tile, tile), tile)
                out = jnp.dot(r["x"][...], r["w"][l, :, at], preferred_element_type=jnp.float32)
                mine = pl.ds(pl.multiple_of(place * cols + t * tile, tile), tile)
                r["b"][l, rows_of(c), mine] = out.astype(jnp.bfloat16)
                return carry

            lax.fori_loop(0, tiles, dot_body, 0)
            for way in range(2):

                @pl.when(has_sent(way, 0))
                def _():
                    pass_on(l, way, 0, c).start()

            return carry

        lax.fori_loop(0, chunks, chunk_body, 0)
        for hop in range(hops - 1):

            def forward_body(c, carry):
                for way in range(2):

                    @pl.when(has_got(way, hop))
                    def _():
                        pass_on(l, way, hop, c).wait_recv()

                    @pl.when(has_sent(way, hop + 1))
                    def _():
                        pass_on(l, way, hop + 1, c).start()

                return carry

            lax.fori_loop(0, chunks, forward_body, 0)
            if hop == 0:
                gather_mid(l + 1)
        gather_end(l + 1)
        return carry

    lax.fori_loop(0, layers - 1, layer_body, 0)

    last = layers - 1

    def last_body(c, carry):
        add_chunk(last, c)
        norm_chunk(last, c)

        def dot_body(t, carry):
            at = pl.ds(pl.multiple_of(t * tile, tile), tile)
            out = jnp.dot(r["x"][...], r["w"][last, :, at], preferred_element_type=jnp.float32)
            out = out.astype(jnp.bfloat16).astype(jnp.float32)
            mine = pl.ds(pl.multiple_of(place * cols + t * tile, tile), tile)
            slot = c * part + lax.broadcasted_iota(jnp.int32, (part, tile), 0)
            total = r["stream"][rows_of(c), mine] + out
            total = jnp.where(slot < count, total, 0.0)
            r["mixed"][rows_of(c), at] = total.astype(jnp.bfloat16)
            return carry

        lax.fori_loop(0, tiles, dot_body, 0)
        return carry

    lax.fori_loop(0, chunks, last_body, 0)

    def finish_gather(l, carry):
        for way, hop, sub in all_rings():
            ring_copy(l, way, hop, sub).wait_send()
        for owner, slot, sub in all_mates():
            mate_copy(l, owner, slot, sub).wait_send()
        return carry

    lax.fori_loop(0, layers, finish_gather, 0)

    def finish_layer(l, carry):
        def finish_body(c, carry):
            for hop in range(hops):
                for way in range(2):

                    @pl.when(has_sent(way, hop))
                    def _():
                        pass_on(l, way, hop, c).wait_send()

            return carry

        return lax.fori_loop(0, chunks, finish_body, carry)

    lax.fori_loop(0, layers - 1, finish_layer, 0)


def run_layers(sizes, own, tokens, hot, table, gain, counts):
    n_dp, n = sizes
    layers, rows, cols = own.shape
    tok, width = tokens.shape
    chunks = 4
    part = tok // chunks
    half = n_dp // 4
    dma = pltpu.SemaphoreType.DMA
    names = ["own", "tokens", "hot", "table", "gain", "counts", "mixed"]
    scratch = {
        "w": pltpu.VMEM((layers, n_dp * rows, cols), jnp.bfloat16),
        "stream": pltpu.VMEM((tok, width), jnp.float32),
        "b": pltpu.VMEM((layers - 1, tok, width), jnp.bfloat16),
        "x": pltpu.VMEM((part, width), jnp.bfloat16),
        "own_sem": dma((layers,)),
        "tok_sem": dma((1,)),
        "ring_send": dma((layers, 2, half, 2)),
        "ring_recv": dma((layers, 2, half, 2)),
        "mate_send": dma((layers, 1 + 2 * half, 2)),
        "mate_recv": dma((layers, 1 + 2 * half, 2)),
        "send": dma((layers - 1, 2, n - 1, chunks)),
        "recv": dma((layers - 1, 2, n - 1, chunks)),
    }
    return pl.pallas_call(
        functools.partial(layers_kernel, n_dp, n, chunks, names + list(scratch)),
        out_shape=jax.ShapeDtypeStruct((tok, cols), jnp.bfloat16),
        in_specs=[ANY, ANY, VMEM, VMEM, VMEM, SMEM],
        out_specs=VMEM,
        scratch_shapes=list(scratch.values()),
        compiler_params=pltpu.CompilerParams(
            collective_id=1, has_side_effects=True, vmem_limit_bytes=63 * 2**20
        ),
        name="layers",
    )(own, tokens, hot, table, gain[:, None, :], counts)


def code_table(width):
    quarter = width // 4
    freqs = 1.0 / 10000.0 ** (jnp.arange(quarter, dtype=jnp.float32) / quarter)
    angle = jnp.arange(GRID, dtype=jnp.float32)[:, None] * freqs[None, :]
    exact = jnp.concatenate([jnp.sin(angle), jnp.cos(angle)], axis=1)
    high = lax.reduce_precision(exact, 8, 7)
    middle = lax.reduce_precision(exact - high, 8, 7)
    low = exact - high - middle
    lane = jnp.zeros((GRID, 2 * quarter), jnp.float32)
    rows = jnp.concatenate([high, middle, low, lane], axis=0).astype(jnp.bfloat16)
    empty = jnp.zeros_like(rows)
    return jnp.concatenate(
        [jnp.concatenate([rows, empty], axis=1), jnp.concatenate([empty, rows], axis=1)], axis=0
    )


def one_hot(patch_index):
    lane = lax.broadcasted_iota(jnp.int32, (1, 8 * GRID), 1)
    which = jnp.where(lane < 4 * GRID, patch_index[:, None] // GRID, patch_index[:, None] % GRID)
    return (lane % GRID == which).astype(jnp.bfloat16)


def per_device(
    sizes,
    tokens,
    counts,
    patch_index,
    clip_limit,
    norm_gain,
    params,
    moments,
    seconds,
    gradients,
):
    factor, head = total_over_mesh(sizes, clip_limit, gradients, params, moments, seconds)
    params_new, moments_new, seconds_new, own = adam_all(
        factor, params, moments, seconds, gradients
    )
    table = code_table(tokens.shape[1])
    hot = one_hot(patch_index)
    mixed = run_layers(sizes, own, tokens, hot, table, norm_gain, counts)
    return (params_new, moments_new, seconds_new, mixed)


def solution(mesh):
    sizes = (mesh.shape["dp"], mesh.shape["fsdp"])
    weight = P(None, "dp", "fsdp")
    return jax.shard_map(
        functools.partial(per_device, sizes),
        mesh=mesh,
        in_specs=(P("dp", None), P("dp"), P("dp"), P(), P(), weight, weight, weight, weight),
        out_specs=(weight, weight, weight, P("dp", "fsdp")),
        check_vma=False,
    )
```

```python
import functools
import jax
import jax.numpy as jnp
from jax import lax
from jax.experimental import pallas as pl
from jax.experimental.pallas import tpu as pltpu
from jax.sharding import PartitionSpec as P

GRID = 16
STEP = 40

beta_one = 0.9
beta_two = 0.95
adam_eps = 1e-08
learning_rate = 0.0024
weight_decay = 0.05
norm_eps = 1e-06

MESH = pl.DeviceIdType.MESH
ANY = pl.BlockSpec(memory_space=pl.ANY)
VMEM = pl.BlockSpec(memory_space=pltpu.VMEM)
SMEM = pl.BlockSpec(memory_space=pltpu.SMEM)


def adam_update(params, moments, seconds, gradients, factor):
    clipped = gradients * factor
    moments_new = beta_one * moments + (1.0 - beta_one) * clipped
    seconds_new = beta_two * seconds + (1.0 - beta_two) * clipped * clipped
    spread = seconds_new * (1.0 / (1.0 - beta_two**STEP))
    direction = (moments_new * (1.0 / (1.0 - beta_one**STEP))) / (
        spread * lax.rsqrt(spread) + adam_eps
    )
    params_new = params - learning_rate * (direction + weight_decay * params)
    return (params_new, moments_new, seconds_new)


def total_kernel(sizes, chunks, clip_ref, g_ref, p_ref, m_ref, s_ref, factor_ref, head_ref, *scratch):
    g, p, m, s, mine, mid, got0, got1 = scratch[:8]
    g_sem, a_sem, send0, send1, recv0, recv1 = scratch[8:]
    names, got, send, recv = ("dp", "fsdp"), (got0, got1), (send0, send1), (recv0, recv1)
    place = [lax.axis_index(name) for name in names]
    layers, rows, cols = g.shape
    part = rows // chunks

    def take_gradients(l, c):
        at = pl.ds(pl.multiple_of(c * part, part), part)
        return pltpu.make_async_copy(g_ref.at[l, at], g.at[l, at], g_sem.at[l, c])

    def start_layer(l, carry):
        lax.fori_loop(0, chunks, lambda c, x: (take_gradients(l, c).start(), x)[1], 0)
        return carry

    lax.fori_loop(0, layers, start_layer, 0)
    heads = [
        pltpu.make_async_copy(ref.at[0], to, a_sem.at[i])
        for i, (ref, to) in enumerate(((p_ref, p), (m_ref, m), (s_ref, s)))
    ]
    for copy in heads:
        copy.start()
    barrier = pltpu.get_barrier_semaphore()
    for axis in range(2):
        for step in range(1, sizes[axis]):
            pl.semaphore_signal(
                barrier,
                inc=1,
                device_id={names[axis]: lax.rem(place[axis] + step, sizes[axis])},
                device_id_type=MESH,
            )

    def add_layer(l, total):
        def add_chunk(c, total):
            take_gradients(l, c).wait()

            def add_rows(k, total):
                x = g[l, pl.ds(pl.multiple_of(c * part + k * 32, 32), 32)]
                x = x * x
                sums = [x[8 * i : 8 * i + 8] for i in range(4)]
                y = (sums[0] + sums[1]) + (sums[2] + sums[3])
                return total + y

            return lax.fori_loop(0, part // 32, add_rows, total)

        return lax.fori_loop(0, chunks, add_chunk, total)

    wide = lax.fori_loop(0, layers, add_layer, jnp.zeros((8, cols), jnp.float32))
    total = wide[:, 0:128]
    for k in range(1, cols // 128):
        total = total + wide[:, 128 * k : 128 * k + 128]
    mine[...] = total

    pl.semaphore_wait(barrier, sizes[0] + sizes[1] - 2)
    for axis in range(2):
        source = mine if axis == 0 else mid
        copies = []
        for step in range(1, sizes[axis]):
            copy = pltpu.make_async_remote_copy(
                src_ref=source,
                dst_ref=got[axis].at[place[axis]],
                send_sem=send[axis].at[step - 1],
                recv_sem=recv[axis].at[step - 1],
                device_id={names[axis]: lax.rem(place[axis] + step, sizes[axis])},
                device_id_type=MESH,
            )
            copy.start()
            copies.append(copy)
        got[axis][place[axis]] = source[...]
        for copy in copies:
            copy.wait()
        total = got[axis][0]
        for slot in range(1, sizes[axis]):
            total = total + got[axis][slot]
        if axis == 0:
            mid[...] = total
    squares = jnp.sum(jnp.sum(total, axis=1, keepdims=True), axis=0, keepdims=True)
    factor = jnp.minimum(1.0, clip_ref[0] / (jnp.sqrt(squares) + 1e-06))
    factor_ref[...] = jnp.broadcast_to(factor, factor_ref.shape)
    for copy in heads:
        copy.wait()

    def update(k, carry):
        at = pl.ds(pl.multiple_of(k * 16, 16), 16)
        head_ref[at] = adam_update(p[at], m[at], s[at], g[0, at], factor)[0].astype(jnp.bfloat16)
        return carry

    lax.fori_loop(0, rows // 16, update, 0)


def total_over_mesh(sizes, clip_limit, gradients, params, moments, seconds):
    layers, rows, cols = gradients.shape
    shape, f32, dma = (8, 128), jnp.float32, pltpu.SemaphoreType.DMA
    chunks = 2
    return pl.pallas_call(
        functools.partial(total_kernel, sizes, chunks),
        out_shape=[
            jax.ShapeDtypeStruct((8, 128), f32),
            jax.ShapeDtypeStruct((rows, cols), jnp.bfloat16),
        ],
        in_specs=[SMEM, ANY, ANY, ANY, ANY],
        out_specs=[VMEM, VMEM],
        scratch_shapes=[pltpu.VMEM((layers, rows, cols), f32)]
        + [pltpu.VMEM((rows, cols), f32)] * 3
        + [pltpu.VMEM(shape, f32)] * 2
        + [pltpu.VMEM((size,) + shape, f32) for size in sizes]
        + [dma((layers, chunks)), dma((3,))]
        + [dma((max(size - 1, 1),)) for size in sizes] * 2,
        compiler_params=pltpu.CompilerParams(
            collective_id=0, has_side_effects=True, vmem_limit_bytes=63 * 2**20
        ),
        name="total",
    )(clip_limit[None], gradients, params, moments, seconds)


def adam_kernel(f_ref, p_ref, m_ref, s_ref, g_ref, po_ref, mo_ref, so_ref, w_ref):
    factor = f_ref[0:1, 0:1]

    def update(k, carry):
        at = pl.ds(pl.multiple_of(k * 16, 16), 16)
        new = adam_update(p_ref[0, at], m_ref[0, at], s_ref[0, at], g_ref[0, at], factor)
        po_ref[0, at], mo_ref[0, at], so_ref[0, at] = new
        w_ref[0, at] = new[0].astype(jnp.bfloat16)
        return carry

    lax.fori_loop(0, p_ref.shape[1] // 16, update, 0)


def adam_all(factor, params, moments, seconds, gradients):
    layers, rows, cols = params.shape
    part = 128
    block = pl.BlockSpec((1, part, cols), lambda l, c: (l, c, 0))
    f32 = jax.ShapeDtypeStruct(params.shape, jnp.float32)
    return pl.pallas_call(
        adam_kernel,
        grid=(layers, rows // part),
        out_shape=[f32, f32, f32, jax.ShapeDtypeStruct(params.shape, jnp.bfloat16)],
        in_specs=[pl.BlockSpec((8, 128), lambda l, c: (0, 0))] + [block] * 4,
        out_specs=[block] * 4,
        compiler_params=pltpu.CompilerParams(vmem_limit_bytes=63 * 2**20),
        cost_estimate=pl.CostEstimate(
            flops=20 * params.size, bytes_accessed=30 * params.size, transcendentals=0
        ),
        name="adam",
    )(factor, params, moments, seconds, gradients)


def layers_kernel(n_dp, n, chunks, names, *refs):
    r = dict(zip(names, refs))
    layers, rows, cols = r["own"].shape
    tok, width = r["stream"].shape
    part = tok // chunks
    tile = min(256, cols)
    tiles = cols // tile
    sub_rows = rows // 2
    ring = n_dp // 2
    half = ring // 2
    hops = n - 1
    sub = 32
    split = 2
    last = layers - 1
    dp, place = lax.axis_index("dp"), lax.axis_index("fsdp")
    chip, core = dp // 2, lax.rem(dp, 2)
    count = r["counts"][0]

    side = place // (n // 2)
    end = side * (n - 1)
    middle = n // 2 - 1 + side
    inner = jnp.logical_and(place > 0, place < n - 1)
    outer = jnp.logical_not(inner)

    def turn(i):
        if ring != 4:
            return i
        return (i // 2) * 2 + lax.rem(i + i // 2, 2)

    pos = turn(chip)

    def dp_of(position, which):
        return turn(lax.rem(position + 2 * ring, ring)) * 2 + which

    def w_rows(position, sub):
        at = dp_of(position, core) * rows + sub * sub_rows
        return pl.ds(pl.multiple_of(at, sub_rows), sub_rows)

    def rows_of(c):
        return pl.ds(pl.multiple_of(c * part, part), part)

    def cols_of(owner):
        return pl.ds(pl.multiple_of(owner * cols, cols), cols)

    everything = pl.ds(0, cols)
    first_cols = cols // 8 * 5
    by_z = pl.ds(0, first_cols)
    by_ring = pl.ds(first_cols, cols - first_cols)
    next_chip = {"dp": dp_of(pos + 1, core)}
    last_chip = {"dp": dp_of(pos - 1, core)}
    mate = {"dp": chip * 2 + 1 - core}

    def spare(l):
        return 0 if l == last else layers + l - split

    def take_own(l):
        return pltpu.make_async_copy(
            r["own"].at[l],
            r["w"].at[l, pl.ds(pl.multiple_of(dp * rows, rows), rows)],
            r["own_sem"].at[l],
        )

    def take_near(way):
        owner = came(way, 0)
        at = pl.ds(pl.multiple_of(dp_of(owner, core) * rows, rows), rows)
        return pltpu.make_async_copy(
            r["from_last" if way == 0 else "from_next"], r["w"].at[0, at], r["near_sem"].at[way]
        )

    def send_rows(to, source, target, owner, sub, which, send, recv):
        at = w_rows(owner, sub)
        return pltpu.make_async_remote_copy(
            src_ref=r["w"].at[source, at, which],
            dst_ref=r["w"].at[target, at, which],
            send_sem=send,
            recv_sem=recv,
            device_id=to,
            device_id_type=MESH,
        )

    def came(way, hop):
        return pos - 1 - hop if way == 0 else pos + 1 + hop

    ring_order = ((0, 0), (1, 1), (0, 1), (1, 0))

    def arrivals(hop):
        return [(way, sub) for way, sub in ring_order if hop < half - 1 or sub == way]

    class Gather:
        def __init__(self, slot, index, which):
            self.slot, self.index, self.which = slot, index, which

        def ring(self, way, hop, sub):
            at = (self.index, way, hop, sub)
            return send_rows(
                next_chip if way == 0 else last_chip,
                self.slot,
                self.slot,
                pos - hop if way == 0 else pos + hop,
                sub,
                self.which,
                r["ring_send"].at[at],
                r["ring_recv"].at[at],
            )

        def mate(self, owner, slot, sub):
            at = (self.index, slot, sub)
            return send_rows(
                mate,
                self.slot,
                self.slot,
                owner,
                sub,
                self.which,
                r["mate_send"].at[at],
                r["mate_recv"].at[at],
            )

        def blocks(self):
            out = [(pos, 0, 0), (pos, 0, 1)]
            for hop in range(half):
                out += [(came(way, hop), 1 + 2 * hop + way, sub) for way, sub in arrivals(hop)]
            return out

        def start_ring(self):
            for way, sub in arrivals(0):
                self.ring(way, 0, sub).start()

        def start(self):
            self.start_ring()
            for sub in range(2):
                self.mate(pos, 0, sub).start()

        def step(self, hop, relay, arrived=None):
            for way, sub in arrivals(hop):
                if arrived is None:
                    self.ring(way, hop, sub).wait_recv()
                elif sub == way:
                    arrived(way)
                if hop + 1 < half and (way, sub) in arrivals(hop + 1):
                    self.ring(way, hop + 1, sub).start()
                if relay is not None:
                    relay(came(way, hop), 1 + 2 * hop + way, sub).start()

        def mid(self, relay=None):
            for hop in range(half - 1):
                self.step(hop, relay or self.mate)

        def finish(self, relay=None):
            self.step(half - 1, relay or self.mate)

        def wait_mates(self):
            for owner, slot, sub in self.blocks():
                self.mate(owner, slot, sub).wait_recv()

        def end(self):
            self.finish()
            self.wait_mates()

        def sent_ring(self, first=0):
            for hop in range(first, half):
                for way, sub in arrivals(hop):
                    self.ring(way, hop, sub).wait_send()

        def sent_mates(self):
            for owner, slot, sub in self.blocks():
                self.mate(owner, slot, sub).wait_send()

    class Across(Gather):
        def __init__(self, l):
            self.l, self.to = l, {"fsdp": middle}
            self.a = Gather(spare(l), layers + l - split, by_z)
            self.b = Gather(spare(l), layers + l - split, by_ring)
            self.out = Gather(l, layers + l - split, by_ring)

        def sems(self, slot, sub):
            at = (self.l - split, slot, sub)
            return r["across_send"].at[at], r["across_recv"].at[at]

        def first(self, sub):
            pair = self.sems(ring + 1, sub)
            return send_rows(self.to, self.l, spare(self.l), pos, sub, by_z, *pair)

        def open_first(self):
            for sub in range(2):
                self.first(sub).start()

        def relay_own(self):
            for sub in range(2):
                self.relay(pos, 0, sub).start()

        def relay(self, owner, slot, sub):
            pair = self.sems(slot, sub)
            return send_rows(self.to, self.l, spare(self.l), owner, sub, by_ring, *pair)

        def mate_b(self, owner, slot, sub):
            at = (self.l - split, slot, sub)
            return send_rows(
                mate,
                spare(self.l),
                spare(self.l),
                owner,
                sub,
                by_ring,
                r["again_send"].at[at],
                r["again_recv"].at[at],
            )

    gathers = [Gather(l, l, everything) for l in range(layers)]
    across = {l: Across(l) for l in range(split, layers)}

    def pass_on(l, way, hop, c):
        owner = place - hop if way == 0 else place + hop
        peer = lax.rem(place + 1, n) if way == 0 else lax.rem(place + n - 1, n)
        target = r["b"].at[l % 2, rows_of(c), cols_of(owner)]
        return pltpu.make_async_remote_copy(
            src_ref=target,
            dst_ref=target,
            send_sem=r["send"].at[l, way, hop, c],
            recv_sem=r["recv"].at[l, way, hop, c],
            device_id={"fsdp": peer},
            device_id_type=MESH,
        )

    def has_sent(l, way, hop):
        if way == 0:
            near = place < (n - 1 if l + 1 < split else n - 2)
            far = place >= hop
        else:
            near = place > (0 if l + 1 < split else 1)
            far = place + hop < n
        both = jnp.logical_and(near, far)
        return jnp.logical_and(both, inner) if l >= split else both

    def has_got(l, way, hop):
        if way == 0:
            near = place <= (n - 1 if l + 1 < split else n - 2)
            far = place >= hop + 1
        else:
            near = place >= (0 if l + 1 < split else 1)
            far = place + hop + 1 < n
        both = jnp.logical_and(near, far)
        if l >= split:
            both = jnp.logical_and(both, place >= n // 2 if way == 0 else place < n // 2)
            both = jnp.logical_and(both, inner)
        return both

    def give_mixed(c):
        return pltpu.make_async_remote_copy(
            src_ref=r["b"].at[1, rows_of(c), cols_of(end)],
            dst_ref=r["mixed"].at[rows_of(c)],
            send_sem=r["mixed_send"].at[c],
            recv_sem=r["mixed_recv"].at[c],
            device_id={"fsdp": jnp.where(inner, end, middle)},
            device_id_type=MESH,
        )

    take_tokens = pltpu.make_async_copy(r["tokens"], r["b"].at[1], r["tok_sem"].at[0])
    for l in range(layers):
        take_own(l).start()
    for way in range(2):
        take_near(way).start()
    take_tokens.start()

    barrier = pltpu.get_barrier_semaphore()
    peers = [{"fsdp": lax.rem(place + 1, n)}, {"fsdp": lax.rem(place + n - 1, n)}]
    peers += [next_chip, last_chip, mate]
    for peer in peers:
        pl.semaphore_signal(barrier, inc=1, device_id=peer, device_id_type=MESH)
    pl.semaphore_wait(barrier, len(peers))

    for l in range(layers):
        take_own(l).wait()
    opening = gathers[0]
    opening.step(0, opening.mate, lambda way: take_near(way).wait())
    for half_block in range(2):
        opening.mate(pos, 0, half_block).start()
    gathers[1].start()

    @pl.when(outer)
    def _():
        across[split].open_first()

    take_tokens.wait()

    def init_body(t, carry):
        at = pl.ds(pl.multiple_of(t * tile, tile), tile)
        code = jnp.dot(r["hot"][...], r["table"][:, at], preferred_element_type=jnp.float32)
        slot = lax.broadcasted_iota(jnp.int32, code.shape, 0)
        value = r["b"][1, :, at].astype(jnp.float32) + code
        r["stream"][:, at] = jnp.where(slot < count, value, 0.0)
        return carry

    with jax.named_scope("init"):
        lax.fori_loop(0, width // tile, init_body, 0)
    with jax.named_scope("opening"):
        for hop in range(1, half - 1):
            opening.step(hop, opening.mate)
        opening.end()

    def norm_chunk(l, c):
        def norm_body(k, carry):
            at = pl.ds(pl.multiple_of(c * part + k * sub, sub), sub)
            x = r["stream"][at]
            centre = jnp.sum(x, axis=1, keepdims=True) * (1.0 / width)
            shifted = x - centre
            spread = jnp.sum(shifted * shifted, axis=1, keepdims=True) * (1.0 / width)
            normed = shifted * lax.rsqrt(spread + norm_eps) * r["gain"][l]
            r["x"][at] = normed.astype(jnp.bfloat16)
            return carry

        lax.fori_loop(0, part // sub, norm_body, 0)

    def add_chunk(l, c):
        def add_body(k, carry):
            at = pl.ds(pl.multiple_of(c * part + k * sub, sub), sub)
            r["stream"][at] = r["stream"][at] + r["b"][(l - 1) % 2, at].astype(jnp.float32)
            return carry

        lax.fori_loop(0, part // sub, add_body, 0)

    def wait_pieces(l, hop, c):
        for way in range(2):

            @pl.when(has_got(l, way, hop))
            def _():
                pass_on(l, way, hop, c).wait_recv()

    def send_piece(l, hop, c):
        for way in range(2):

            @pl.when(has_sent(l, way, hop))
            def _():
                pass_on(l, way, hop, c).start()

    def multiply(slot, at_rows, take):
        def dot_body(t, carry):
            at = pl.ds(pl.multiple_of(t * tile, tile), tile)
            out = jnp.dot(
                r["x"][at_rows], r["w"][slot, :, at], preferred_element_type=jnp.float32
            )
            take(t, at, out.astype(jnp.bfloat16))
            return carry

        lax.fori_loop(0, tiles, dot_body, 0)

    def branch_into(l, c, owner):
        def take(t, at, out):
            mine = pl.ds(pl.multiple_of(owner * cols + t * tile, tile), tile)
            r["b"][l % 2, rows_of(c), mine] = out

        return take

    def branch(l, slot, c, owner):
        multiply(slot, rows_of(c), branch_into(l, c, owner))

    def result(slot, at_rows, start, owner, put):
        def take(t, at, out):
            mine = pl.ds(pl.multiple_of(owner * cols + t * tile, tile), tile)
            place_of = start + lax.broadcasted_iota(jnp.int32, out.shape, 0)
            total = r["stream"][at_rows, mine] + out.astype(jnp.float32)
            put(mine, at, jnp.where(place_of < count, total, 0.0).astype(jnp.bfloat16))

        multiply(slot, at_rows, take)

    def over_chunks(body, low=0, high=chunks):
        lax.fori_loop(low, high, lambda c, carry: (body(c), carry)[1], 0)

    def sent_chunk(l, c):
        for hop in range(hops):
            for way in range(2):

                @pl.when(has_sent(l, way, hop))
                def _():
                    pass_on(l, way, hop, c).wait_send()

    def sent_pieces(l):
        over_chunks(lambda c: sent_chunk(l, c))

    @pl.when(outer)
    def _():
        across[split].out.start_ring()

    def body(c):
        norm_chunk(0, c)
        branch(0, 0, c, place)
        send_piece(0, 0, c)

    with jax.named_scope("layer_0"):
        over_chunks(body)
    opening.sent_ring(1)
    opening.sent_mates()

    @pl.when(inner)
    def _():
        for peer in (next_chip, last_chip, mate, {"fsdp": end}):
            pl.semaphore_signal(r["free"], inc=1, device_id=peer, device_id_type=MESH)

    def forward(l, hop, low=0, high=chunks):
        def body(c):
            if l + 1 == split:
                sent_chunk(l - 1, c)
            wait_pieces(l, hop, c)
            send_piece(l, hop + 1, c)

        over_chunks(body, low, high)

    def layer_one(c):
        add_chunk(1, c)
        norm_chunk(1, c)
        branch(1, 1, c, place)
        send_piece(1, 0, c)

    both_halves = range(2)

    @pl.when(outer)
    def _():
        with jax.named_scope("outer_gather"):
            gathers[1].mid()
        with jax.named_scope("outer_feed"):
            across[split].relay_own()
            across[split].out.mid(across[split].relay)
            gathers[1].finish()
            across[split].out.finish(across[split].relay)
            across[last].out.start_ring()
            pl.semaphore_wait(r["free"], 1)
            gathers[1].wait_mates()

        def body(c):
            for hop in range(hops):
                wait_pieces(0, hop, c)
            layer_one(c)

        with jax.named_scope("outer_layer_1"):
            over_chunks(body)
        with jax.named_scope("outer_sent"):
            sent_pieces(1)
        with jax.named_scope("outer_feeds"):
            across[last].open_first()
            across[last].relay_own()
            across[last].out.mid(across[last].relay)
            across[last].out.finish(across[last].relay)
        with jax.named_scope("outer_mixed"):
            over_chunks(lambda c: give_mixed(c).wait_recv())
        for l in range(split, layers):
            for half_block in both_halves:
                across[l].first(half_block).wait_send()
            across[l].out.sent_ring()
            for owner, slot, half_block in across[l].out.blocks():
                across[l].relay(owner, slot, half_block).wait_send()
        sent_pieces(0)

    def open_spare(l):
        if l == last:
            pl.semaphore_wait(r["free"], 3)
        for half_block in both_halves:
            across[l].first(half_block).wait_recv()
        across[l].a.start()

    def relay_spare(l):
        blocks = across[l].b.blocks()
        for owner, slot, half_block in blocks:
            across[l].relay(owner, slot, half_block).wait_recv()
            across[l].mate_b(owner, slot, half_block).start()

    def wait_spare(l):
        across[l].a.wait_mates()
        for owner, slot, half_block in across[l].b.blocks():
            across[l].mate_b(owner, slot, half_block).wait_recv()

    @pl.when(inner)
    def _():
        with jax.named_scope("forward_0"):
            forward(0, 0, 0, chunks - 1)
        with jax.named_scope("gather_1_mid"):
            gathers[1].mid()
        with jax.named_scope("forward_0b"):
            forward(0, 0, chunks - 1, chunks)
        with jax.named_scope("forward_1"):
            forward(0, 1, 0, chunks // 2)
        gathers[split].start()
        open_spare(split)
        with jax.named_scope("forward_1b"):
            forward(0, 1, chunks // 2, chunks)
        with jax.named_scope("gather_1_end"):
            gathers[1].end()
        with jax.named_scope("layer_1"):
            over_chunks(layer_one)
        with jax.named_scope("gather_2_mid"):
            gathers[split].mid()
            across[split].a.mid()
        with jax.named_scope("forward_2"):
            forward(1, 0, 0, chunks // 2)
        with jax.named_scope("spare_relay"):
            relay_spare(split)
        with jax.named_scope("forward_2b"):
            forward(1, 0, chunks // 2, chunks)
        gathers[last].start()
        with jax.named_scope("gather_2_end"):
            gathers[split].finish()
            across[split].a.finish()
        with jax.named_scope("spare_open"):
            open_spare(last)
        with jax.named_scope("wait_mates"):
            gathers[split].wait_mates()
            wait_spare(split)

        def body(c):
            wait_pieces(1, 1, c)
            add_chunk(split, c)
            norm_chunk(split, c)
            branch(split, split, c, place)
            send_piece(split, 0, c)
            branch(split, spare(split), c, end)
            send_piece(split, 1, c)

        with jax.named_scope("layer_2"):
            over_chunks(body)
        with jax.named_scope("last_mid"):
            across[last].a.mid()
            gathers[last].mid()
        with jax.named_scope("last_relay"):
            relay_spare(last)
        with jax.named_scope("last_spare"):
            across[last].a.finish()
            wait_spare(last)
            sent_pieces(1)

        def put_away(c):
            def put(mine, at, value):
                r["b"][1, rows_of(c), mine] = value

            return put

        def put_here(mine, at, value):
            r["mixed"][:, at] = value

        def body(c):
            wait_pieces(last - 1, 0, c)
            wait_pieces(last - 1, 1, c)
            add_chunk(last, c)
            norm_chunk(last, c)
            result(spare(last), rows_of(c), c * part, end, put_away(c))
            give_mixed(c).start()

        with jax.named_scope("layer_3"):
            over_chunks(body)
        with jax.named_scope("last_gather_end"):
            gathers[last].end()
        with jax.named_scope("layer_3_own"):
            result(last, pl.ds(0, tok), 0, place, put_here)
        sent_pieces(last - 1)
        for l in range(split, layers):
            gathers[l].sent_ring()
            gathers[l].sent_mates()
            across[l].a.sent_ring()
            across[l].a.sent_mates()
            for owner, slot, half_block in across[l].b.blocks():
                across[l].mate_b(owner, slot, half_block).wait_send()
        over_chunks(lambda c: give_mixed(c).wait_send())

    gathers[1].sent_ring()
    gathers[1].sent_mates()


def run_layers(sizes, own, from_last, from_next, tokens, hot, table, gain, counts):
    n_dp, n = sizes
    layers, rows, cols = own.shape
    tok, width = tokens.shape
    chunks = 4
    part = tok // chunks
    half = n_dp // 4
    dma = pltpu.SemaphoreType.DMA
    names = ["own", "from_last", "from_next", "tokens", "hot", "table", "gain", "counts", "mixed"]
    scratch = {
        "w": pltpu.VMEM((layers + 1, n_dp * rows, cols), jnp.bfloat16),
        "stream": pltpu.VMEM((tok, width), jnp.float32),
        "b": pltpu.VMEM((2, tok, width), jnp.bfloat16),
        "x": pltpu.VMEM((tok, width), jnp.bfloat16),
        "own_sem": dma((layers,)),
        "near_sem": dma((2,)),
        "tok_sem": dma((1,)),
        "ring_send": dma((layers + 2, 2, half, 2)),
        "ring_recv": dma((layers + 2, 2, half, 2)),
        "mate_send": dma((layers + 2, 1 + 2 * half, 2)),
        "mate_recv": dma((layers + 2, 1 + 2 * half, 2)),
        "across_send": dma((2, 2 + 2 * half, 2)),
        "across_recv": dma((2, 2 + 2 * half, 2)),
        "again_send": dma((2, 1 + 2 * half, 2)),
        "again_recv": dma((2, 1 + 2 * half, 2)),
        "send": dma((layers - 1, 2, n - 1, chunks)),
        "recv": dma((layers - 1, 2, n - 1, chunks)),
        "mixed_send": dma((chunks,)),
        "mixed_recv": dma((chunks,)),
        "free": pltpu.SemaphoreType.REGULAR,
    }
    return pl.pallas_call(
        functools.partial(layers_kernel, n_dp, n, chunks, names + list(scratch)),
        out_shape=jax.ShapeDtypeStruct((tok, cols), jnp.bfloat16),
        in_specs=[ANY, ANY, ANY, ANY, VMEM, VMEM, VMEM, SMEM],
        out_specs=VMEM,
        scratch_shapes=list(scratch.values()),
        compiler_params=pltpu.CompilerParams(
            collective_id=1, has_side_effects=True, vmem_limit_bytes=67043328
        ),
        name="layers",
    )(own, from_last, from_next, tokens, hot, table, gain[:, None, :], counts)


def ring_pairs(n_dp):
    ring = n_dp // 2
    order = [0, 1, 3, 2] if ring == 4 else list(range(ring))
    return [
        (2 * order[i] + core, 2 * order[(i + 1) % ring] + core)
        for i in range(ring)
        for core in range(2)
    ]


def code_table(width):
    quarter = width // 4
    freqs = 1.0 / 10000.0 ** (jnp.arange(quarter, dtype=jnp.float32) / quarter)
    angle = jnp.arange(GRID, dtype=jnp.float32)[:, None] * freqs[None, :]
    exact = jnp.concatenate([jnp.sin(angle), jnp.cos(angle)], axis=1)
    high = lax.reduce_precision(exact, 8, 7)
    middle = lax.reduce_precision(exact - high, 8, 7)
    low = exact - high - middle
    lane = jnp.zeros((GRID, 2 * quarter), jnp.float32)
    rows = jnp.concatenate([high, middle, low, lane], axis=0).astype(jnp.bfloat16)
    empty = jnp.zeros_like(rows)
    return jnp.concatenate(
        [jnp.concatenate([rows, empty], axis=1), jnp.concatenate([empty, rows], axis=1)], axis=0
    )


def one_hot(patch_index):
    lane = lax.broadcasted_iota(jnp.int32, (1, 8 * GRID), 1)
    which = jnp.where(lane < 4 * GRID, patch_index[:, None] // GRID, patch_index[:, None] % GRID)
    return (lane % GRID == which).astype(jnp.bfloat16)


def per_device(
    sizes,
    tokens,
    counts,
    patch_index,
    clip_limit,
    norm_gain,
    params,
    moments,
    seconds,
    gradients,
):
    factor, head = total_over_mesh(sizes, clip_limit, gradients, params, moments, seconds)
    pairs = ring_pairs(sizes[0])
    from_last = lax.ppermute(head, "dp", pairs)
    from_next = lax.ppermute(head, "dp", [(target, source) for source, target in pairs])
    params_new, moments_new, seconds_new, own = adam_all(
        factor, params, moments, seconds, gradients
    )
    table = code_table(tokens.shape[1])
    hot = one_hot(patch_index)
    mixed = run_layers(
        sizes, own, from_last, from_next, tokens, hot, table, norm_gain, counts
    )
    return (params_new, moments_new, seconds_new, mixed)


def solution(mesh):
    sizes = (mesh.shape["dp"], mesh.shape["fsdp"])
    weight = P(None, "dp", "fsdp")
    return jax.shard_map(
        functools.partial(per_device, sizes),
        mesh=mesh,
        in_specs=(P("dp", None), P("dp"), P("dp"), P(), P(), weight, weight, weight, weight),
        out_specs=(weight, weight, weight, P("dp", "fsdp")),
        check_vma=False,
    )
```

```python
import functools
import jax
import jax.numpy as jnp
from jax import lax
from jax.experimental import pallas as pl
from jax.experimental.pallas import tpu as pltpu
from jax.sharding import PartitionSpec as P

GRID = 16
STEP = 40

beta_one = 0.9
beta_two = 0.95
adam_eps = 1e-08
learning_rate = 0.0024
weight_decay = 0.05
norm_eps = 1e-06

MESH = pl.DeviceIdType.MESH
ANY = pl.BlockSpec(memory_space=pl.ANY)
VMEM = pl.BlockSpec(memory_space=pltpu.VMEM)
SMEM = pl.BlockSpec(memory_space=pltpu.SMEM)


def adam_update(params, moments, seconds, gradients, factor):
    clipped = gradients * factor
    moments_new = beta_one * moments + (1.0 - beta_one) * clipped
    seconds_new = beta_two * seconds + (1.0 - beta_two) * clipped * clipped
    spread = seconds_new * (1.0 / (1.0 - beta_two**STEP))
    direction = (moments_new * (1.0 / (1.0 - beta_one**STEP))) / (
        spread * lax.rsqrt(spread) + adam_eps
    )
    params_new = params - learning_rate * (direction + weight_decay * params)
    return (params_new, moments_new, seconds_new)


def total_kernel(sizes, chunks, clip_ref, g_ref, p_ref, m_ref, s_ref, factor_ref, head_ref, *scratch):
    g, p, m, s, mine, mid, got0, got1 = scratch[:8]
    g_sem, a_sem, send0, send1, recv0, recv1 = scratch[8:]
    names, got, send, recv = ("dp", "fsdp"), (got0, got1), (send0, send1), (recv0, recv1)
    place = [lax.axis_index(name) for name in names]
    layers, rows, cols = g.shape
    part = rows // chunks

    def take_gradients(l, c):
        at = pl.ds(pl.multiple_of(c * part, part), part)
        return pltpu.make_async_copy(g_ref.at[l, at], g.at[l, at], g_sem.at[l, c])

    def start_layer(l, carry):
        lax.fori_loop(0, chunks, lambda c, x: (take_gradients(l, c).start(), x)[1], 0)
        return carry

    lax.fori_loop(0, layers, start_layer, 0)
    heads = [
        pltpu.make_async_copy(ref.at[0], to, a_sem.at[i])
        for i, (ref, to) in enumerate(((p_ref, p), (m_ref, m), (s_ref, s)))
    ]
    for copy in heads:
        copy.start()
    barrier = pltpu.get_barrier_semaphore()
    for axis in range(2):
        for step in range(1, sizes[axis]):
            pl.semaphore_signal(
                barrier,
                inc=1,
                device_id={names[axis]: lax.rem(place[axis] + step, sizes[axis])},
                device_id_type=MESH,
            )

    def add_layer(l, total):
        def add_chunk(c, total):
            take_gradients(l, c).wait()

            def add_rows(k, total):
                x = g[l, pl.ds(pl.multiple_of(c * part + k * 32, 32), 32)]
                x = x * x
                sums = [x[8 * i : 8 * i + 8] for i in range(4)]
                y = (sums[0] + sums[1]) + (sums[2] + sums[3])
                return total + y

            return lax.fori_loop(0, part // 32, add_rows, total)

        return lax.fori_loop(0, chunks, add_chunk, total)

    with jax.named_scope("add_up"):
        wide = lax.fori_loop(0, layers, add_layer, jnp.zeros((8, cols), jnp.float32))
    total = wide[:, 0:128]
    for k in range(1, cols // 128):
        total = total + wide[:, 128 * k : 128 * k + 128]
    mine[...] = total

    with jax.named_scope("total_barrier"):
        pl.semaphore_wait(barrier, sizes[0] + sizes[1] - 2)
    for axis in range(2):
        source = mine if axis == 0 else mid
        copies = []
        for step in range(1, sizes[axis]):
            copy = pltpu.make_async_remote_copy(
                src_ref=source,
                dst_ref=got[axis].at[place[axis]],
                send_sem=send[axis].at[step - 1],
                recv_sem=recv[axis].at[step - 1],
                device_id={names[axis]: lax.rem(place[axis] + step, sizes[axis])},
                device_id_type=MESH,
            )
            copy.start()
            copies.append(copy)
        got[axis][place[axis]] = source[...]
        for copy in copies:
            copy.wait()
        total = got[axis][0]
        for slot in range(1, sizes[axis]):
            total = total + got[axis][slot]
        if axis == 0:
            mid[...] = total
    squares = jnp.sum(jnp.sum(total, axis=1, keepdims=True), axis=0, keepdims=True)
    factor = jnp.minimum(1.0, clip_ref[0] / (jnp.sqrt(squares) + 1e-06))
    factor_ref[...] = jnp.broadcast_to(factor, factor_ref.shape)
    for copy in heads:
        copy.wait()

    def update(k, carry):
        at = pl.ds(pl.multiple_of(k * 16, 16), 16)
        head_ref[at] = adam_update(p[at], m[at], s[at], g[0, at], factor)[0].astype(jnp.bfloat16)
        return carry

    with jax.named_scope("head_update"):
        lax.fori_loop(0, rows // 16, update, 0)


def total_over_mesh(sizes, clip_limit, gradients, params, moments, seconds):
    layers, rows, cols = gradients.shape
    shape, f32, dma = (8, 128), jnp.float32, pltpu.SemaphoreType.DMA
    chunks = 2
    return pl.pallas_call(
        functools.partial(total_kernel, sizes, chunks),
        out_shape=[
            jax.ShapeDtypeStruct((8, 128), f32),
            jax.ShapeDtypeStruct((rows, cols), jnp.bfloat16),
        ],
        in_specs=[SMEM, ANY, ANY, ANY, ANY],
        out_specs=[VMEM, VMEM],
        scratch_shapes=[pltpu.VMEM((layers, rows, cols), f32)]
        + [pltpu.VMEM((rows, cols), f32)] * 3
        + [pltpu.VMEM(shape, f32)] * 2
        + [pltpu.VMEM((size,) + shape, f32) for size in sizes]
        + [dma((layers, chunks)), dma((3,))]
        + [dma((max(size - 1, 1),)) for size in sizes] * 2,
        compiler_params=pltpu.CompilerParams(
            collective_id=0, has_side_effects=True, vmem_limit_bytes=63 * 2**20
        ),
        name="total",
    )(clip_limit[None], gradients, params, moments, seconds)


def adam_kernel(f_ref, p_ref, m_ref, s_ref, g_ref, po_ref, mo_ref, so_ref, w_ref):
    factor = f_ref[0:1, 0:1]

    def update(k, carry):
        at = pl.ds(pl.multiple_of(k * 16, 16), 16)
        new = adam_update(p_ref[0, at], m_ref[0, at], s_ref[0, at], g_ref[0, at], factor)
        po_ref[0, at], mo_ref[0, at], so_ref[0, at] = new
        w_ref[0, at] = new[0].astype(jnp.bfloat16)
        return carry

    lax.fori_loop(0, p_ref.shape[1] // 16, update, 0)


def adam_all(factor, params, moments, seconds, gradients):
    layers, rows, cols = params.shape
    part = min(512, rows)
    block = pl.BlockSpec((1, part, cols), lambda l, c: (l, c, 0))
    f32 = jax.ShapeDtypeStruct(params.shape, jnp.float32)
    return pl.pallas_call(
        adam_kernel,
        grid=(layers, rows // part),
        out_shape=[f32, f32, f32, jax.ShapeDtypeStruct(params.shape, jnp.bfloat16)],
        in_specs=[pl.BlockSpec((8, 128), lambda l, c: (0, 0))] + [block] * 4,
        out_specs=[block] * 4,
        compiler_params=pltpu.CompilerParams(vmem_limit_bytes=63 * 2**20),
        cost_estimate=pl.CostEstimate(
            flops=20 * params.size, bytes_accessed=30 * params.size, transcendentals=0
        ),
        name="adam",
    )(factor, params, moments, seconds, gradients)


def layers_kernel(n_dp, n, chunks, names, *refs):
    r = dict(zip(names, refs))
    layers, rows, cols = r["own"].shape
    tok, width = r["stream"].shape
    part = tok // chunks
    tile = min(256, cols)
    tiles = cols // tile
    sub_rows = rows // 2
    ring = n_dp // 2
    half = ring // 2
    hops = n - 1
    sub = 32
    split = 2
    last = layers - 1
    dp, place = lax.axis_index("dp"), lax.axis_index("fsdp")
    chip, core = dp // 2, lax.rem(dp, 2)
    count = r["counts"][0]

    side = place // (n // 2)
    end = side * (n - 1)
    middle = n // 2 - 1 + side
    inner = jnp.logical_and(place > 0, place < n - 1)
    outer = jnp.logical_not(inner)

    def turn(i):
        if ring != 4:
            return i
        return (i // 2) * 2 + lax.rem(i + i // 2, 2)

    pos = turn(chip)

    def dp_of(position, which):
        return turn(lax.rem(position + 2 * ring, ring)) * 2 + which

    def w_rows(position, sub):
        at = dp_of(position, core) * rows + sub * sub_rows
        return pl.ds(pl.multiple_of(at, sub_rows), sub_rows)

    def rows_of(c):
        return pl.ds(pl.multiple_of(c * part, part), part)

    def cols_of(owner):
        return pl.ds(pl.multiple_of(owner * cols, cols), cols)

    everything = pl.ds(0, cols)

    def first_cols(l):
        return cols // 8 * (4 if l == last else 5)

    def by_z(l):
        return pl.ds(0, first_cols(l))

    def by_ring(l):
        return pl.ds(first_cols(l), cols - first_cols(l))

    next_chip = {"dp": dp_of(pos + 1, core)}
    last_chip = {"dp": dp_of(pos - 1, core)}
    mate = {"dp": chip * 2 + 1 - core}

    def spare(l):
        return 0 if l == last else layers + l - split

    def take_own(l):
        return pltpu.make_async_copy(
            r["own"].at[l],
            r["w"].at[l, pl.ds(pl.multiple_of(dp * rows, rows), rows)],
            r["own_sem"].at[l],
        )

    def take_near(way):
        owner = came(way, 0)
        at = pl.ds(pl.multiple_of(dp_of(owner, core) * rows, rows), rows)
        return pltpu.make_async_copy(
            r["from_last" if way == 0 else "from_next"], r["w"].at[0, at], r["near_sem"].at[way]
        )

    def send_rows(to, source, target, owner, sub, which, send, recv):
        at = w_rows(owner, sub)
        return pltpu.make_async_remote_copy(
            src_ref=r["w"].at[source, at, which],
            dst_ref=r["w"].at[target, at, which],
            send_sem=send,
            recv_sem=recv,
            device_id=to,
            device_id_type=MESH,
        )

    def came(way, hop):
        return pos - 1 - hop if way == 0 else pos + 1 + hop

    ring_order = ((0, 0), (1, 1), (0, 1), (1, 0))

    def arrivals(hop):
        return [(way, sub) for way, sub in ring_order if hop < half - 1 or sub == way]

    class Gather:
        def __init__(self, slot, index, which):
            self.slot, self.index, self.which = slot, index, which

        def ring(self, way, hop, sub):
            at = (self.index, way, hop, sub)
            return send_rows(
                next_chip if way == 0 else last_chip,
                self.slot,
                self.slot,
                pos - hop if way == 0 else pos + hop,
                sub,
                self.which,
                r["ring_send"].at[at],
                r["ring_recv"].at[at],
            )

        def mate(self, owner, slot, sub):
            at = (self.index, slot, sub)
            return send_rows(
                mate,
                self.slot,
                self.slot,
                owner,
                sub,
                self.which,
                r["mate_send"].at[at],
                r["mate_recv"].at[at],
            )

        def blocks(self):
            out = [(pos, 0, 0), (pos, 0, 1)]
            for hop in range(half):
                out += [(came(way, hop), 1 + 2 * hop + way, sub) for way, sub in arrivals(hop)]
            return out

        def start_ring(self, low=0, high=4):
            for way, sub in arrivals(0)[low:high]:
                self.ring(way, 0, sub).start()

        def start(self, high=4):
            self.start_ring(0, high)
            for sub in range(2):
                self.mate(pos, 0, sub).start()

        def step(self, hop, relay, arrived=None):
            for way, sub in arrivals(hop):
                if arrived is None:
                    self.ring(way, hop, sub).wait_recv()
                elif sub == way:
                    arrived(way)
                if hop + 1 < half and (way, sub) in arrivals(hop + 1):
                    self.ring(way, hop + 1, sub).start()
                if relay is not None:
                    relay(came(way, hop), 1 + 2 * hop + way, sub).start()

        def mid(self, relay=None):
            for hop in range(half - 1):
                self.step(hop, relay or self.mate)

        def finish(self, relay=None):
            self.step(half - 1, relay or self.mate)

        def wait_mates(self):
            for owner, slot, sub in self.blocks():
                self.mate(owner, slot, sub).wait_recv()

        def end(self):
            self.finish()
            self.wait_mates()

        def sent_ring(self, first=0):
            for hop in range(first, half):
                for way, sub in arrivals(hop):
                    self.ring(way, hop, sub).wait_send()

        def sent_mates(self):
            for owner, slot, sub in self.blocks():
                self.mate(owner, slot, sub).wait_send()

    class Across(Gather):
        def __init__(self, l):
            self.l, self.to = l, {"fsdp": middle}
            self.a = Gather(spare(l), layers + l - split, by_z(l))
            self.b = Gather(spare(l), layers + l - split, by_ring(l))
            self.out = Gather(l, layers + l - split, by_ring(l))

        def sems(self, slot, sub):
            at = (self.l - split, slot, sub)
            return r["across_send"].at[at], r["across_recv"].at[at]

        def first(self, sub):
            pair = self.sems(ring + 1, sub)
            return send_rows(self.to, self.l, spare(self.l), pos, sub, by_z(self.l), *pair)

        def open_first(self):
            for sub in range(2):
                self.first(sub).start()

        def relay_own(self):
            for sub in range(2):
                self.relay(pos, 0, sub).start()

        def relay(self, owner, slot, sub):
            pair = self.sems(slot, sub)
            return send_rows(self.to, self.l, spare(self.l), owner, sub, by_ring(self.l), *pair)

        def mate_b(self, owner, slot, sub):
            at = (self.l - split, slot, sub)
            return send_rows(
                mate,
                spare(self.l),
                spare(self.l),
                owner,
                sub,
                by_ring(self.l),
                r["again_send"].at[at],
                r["again_recv"].at[at],
            )

    gathers = [Gather(l, l, everything) for l in range(layers)]
    across = {l: Across(l) for l in range(split, layers)}

    def pass_on(l, way, hop, c):
        owner = place - hop if way == 0 else place + hop
        peer = lax.rem(place + 1, n) if way == 0 else lax.rem(place + n - 1, n)
        target = r["b"].at[l % 2, rows_of(c), cols_of(owner)]
        return pltpu.make_async_remote_copy(
            src_ref=target,
            dst_ref=target,
            send_sem=r["send"].at[l, way, hop, c],
            recv_sem=r["recv"].at[l, way, hop, c],
            device_id={"fsdp": peer},
            device_id_type=MESH,
        )

    def has_sent(l, way, hop):
        if way == 0:
            near = place < (n - 1 if l + 1 < split else n - 2)
            far = place >= hop
        else:
            near = place > (0 if l + 1 < split else 1)
            far = place + hop < n
        both = jnp.logical_and(near, far)
        return jnp.logical_and(both, inner) if l >= split else both

    def has_got(l, way, hop):
        if way == 0:
            near = place <= (n - 1 if l + 1 < split else n - 2)
            far = place >= hop + 1
        else:
            near = place >= (0 if l + 1 < split else 1)
            far = place + hop + 1 < n
        both = jnp.logical_and(near, far)
        if l >= split:
            both = jnp.logical_and(both, place >= n // 2 if way == 0 else place < n // 2)
            both = jnp.logical_and(both, inner)
        return both

    cut = first_cols(last)
    spans = ((0, cut), (cut, cols - cut))

    def give_mixed(c, which):
        low, wide = spans[which]
        at = pl.ds(pl.multiple_of(end * cols + low, 128), wide)
        return pltpu.make_async_remote_copy(
            src_ref=r["b"].at[1, rows_of(c), at],
            dst_ref=r["mixed"].at[rows_of(c), pl.ds(low, wide)],
            send_sem=r["mixed_send"].at[which, c],
            recv_sem=r["mixed_recv"].at[which, c],
            device_id={"fsdp": jnp.where(inner, end, middle)},
            device_id_type=MESH,
        )

    take_tokens = pltpu.make_async_copy(r["tokens"], r["b"].at[1], r["tok_sem"].at[0])
    for l in range(layers):
        take_own(l).start()
    for way in range(2):
        take_near(way).start()
    take_tokens.start()

    barrier = pltpu.get_barrier_semaphore()
    peers = [{"fsdp": lax.rem(place + 1, n)}, {"fsdp": lax.rem(place + n - 1, n)}]
    peers += [next_chip, last_chip, mate]
    for peer in peers:
        pl.semaphore_signal(barrier, inc=1, device_id=peer, device_id_type=MESH)
    pl.semaphore_wait(barrier, len(peers))

    opening = gathers[0]
    opening.step(0, opening.mate, lambda way: take_near(way).wait())
    for l in range(layers):
        take_own(l).wait()
    for half_block in range(2):
        opening.mate(pos, 0, half_block).start()
    gathers[1].start()

    @pl.when(outer)
    def _():
        across[split].open_first()

    take_tokens.wait()

    def init_body(way, t, carry):
        at = pl.ds(pl.multiple_of(t * tile, tile), tile)
        code = jnp.dot(r["hot"][way], r["table"][:, at], preferred_element_type=jnp.float32)
        at = pl.ds(pl.multiple_of(way * (width // 2) + t * tile, tile), tile)
        slot = lax.broadcasted_iota(jnp.int32, code.shape, 0)
        value = r["b"][1, :, at].astype(jnp.float32) + code
        r["stream"][:, at] = jnp.where(slot < count, value, 0.0)
        return carry

    with jax.named_scope("init"):
        for way in range(2):
            lax.fori_loop(0, width // 2 // tile, functools.partial(init_body, way), 0)
    with jax.named_scope("opening"):
        for hop in range(1, half - 1):
            opening.step(hop, opening.mate)
        opening.end()

    def norm_chunk(l, c):
        def norm_body(k, carry):
            at = pl.ds(pl.multiple_of(c * part + k * sub, sub), sub)
            x = r["stream"][at]
            centre = jnp.sum(x, axis=1, keepdims=True) * (1.0 / width)
            shifted = x - centre
            spread = jnp.sum(shifted * shifted, axis=1, keepdims=True) * (1.0 / width)
            normed = shifted * lax.rsqrt(spread + norm_eps) * r["gain"][l : l + 1]
            r["x"][at] = normed.astype(jnp.bfloat16)
            return carry

        lax.fori_loop(0, part // sub, norm_body, 0)

    def add_chunk(l, c):
        def add_body(k, carry):
            at = pl.ds(pl.multiple_of(c * part + k * sub, sub), sub)
            r["stream"][at] = r["stream"][at] + r["b"][(l - 1) % 2, at].astype(jnp.float32)
            return carry

        lax.fori_loop(0, part // sub, add_body, 0)

    def wait_pieces(l, hop, c):
        for way in range(2):

            @pl.when(has_got(l, way, hop))
            def _():
                pass_on(l, way, hop, c).wait_recv()

    def send_piece(l, hop, c):
        for way in range(2):

            @pl.when(has_sent(l, way, hop))
            def _():
                pass_on(l, way, hop, c).start()

    def multiply(slot, at_rows, take):
        def dot_body(t, carry):
            at = pl.ds(pl.multiple_of(t * tile, tile), tile)
            out = jnp.dot(
                r["x"][at_rows], r["w"][slot, :, at], preferred_element_type=jnp.float32
            )
            take(t, at, out.astype(jnp.bfloat16))
            return carry

        lax.fori_loop(0, tiles, dot_body, 0)

    def branch_into(l, c, owner):
        def take(t, at, out):
            mine = pl.ds(pl.multiple_of(owner * cols + t * tile, tile), tile)
            r["b"][l % 2, rows_of(c), mine] = out

        return take

    def branch(l, slot, c, owner):
        multiply(slot, rows_of(c), branch_into(l, c, owner))

    def result(slot, at_rows, start, owner, put, which=None):
        def take(low, at, out):
            mine = pl.ds(pl.multiple_of(owner * cols + low, 128), out.shape[1])
            place_of = start + lax.broadcasted_iota(jnp.int32, out.shape, 0)
            total = r["stream"][at_rows, mine] + out.astype(jnp.float32)
            put(mine, at, jnp.where(place_of < count, total, 0.0).astype(jnp.bfloat16))

        if which is None:
            multiply(slot, at_rows, lambda t, at, out: take(t * tile, at, out))
            return
        low, wide = spans[which]
        for begin in range(low, low + wide, tile):
            at = pl.ds(begin, min(tile, low + wide - begin))
            out = jnp.dot(
                r["x"][at_rows], r["w"][slot, :, at], preferred_element_type=jnp.float32
            )
            take(begin, at, out.astype(jnp.bfloat16))

    def over_chunks(body, low=0, high=chunks):
        lax.fori_loop(low, high, lambda c, carry: (body(c), carry)[1], 0)

    def sent_chunk(l, c):
        for hop in range(hops):
            for way in range(2):

                @pl.when(has_sent(l, way, hop))
                def _():
                    pass_on(l, way, hop, c).wait_send()

    def sent_pieces(l):
        over_chunks(lambda c: sent_chunk(l, c))

    @pl.when(outer)
    def _():
        across[split].out.start_ring()

    def body(c):
        norm_chunk(0, c)
        branch(0, 0, c, place)
        send_piece(0, 0, c)

    with jax.named_scope("layer_0"):
        over_chunks(body)
    opening.sent_ring(1)
    opening.sent_mates()

    @pl.when(inner)
    def _():
        for peer in (next_chip, last_chip, mate, {"fsdp": end}):
            pl.semaphore_signal(r["free"], inc=1, device_id=peer, device_id_type=MESH)

    def forward(l, hop, low=0, high=chunks):
        def body(c):
            if l + 1 == split:
                sent_chunk(l - 1, c)
            wait_pieces(l, hop, c)
            send_piece(l, hop + 1, c)

        over_chunks(body, low, high)

    def layer_one(c):
        add_chunk(1, c)
        norm_chunk(1, c)
        branch(1, 1, c, place)
        send_piece(1, 0, c)

    both_halves = range(2)

    @pl.when(outer)
    def _():
        with jax.named_scope("outer_gather"):
            gathers[1].mid()
        with jax.named_scope("outer_feed"):
            across[split].relay_own()
            across[split].out.mid(across[split].relay)
            gathers[1].finish()
            across[split].out.finish(across[split].relay)
            across[last].out.start_ring()
            pl.semaphore_wait(r["free"], 1)
            gathers[1].wait_mates()

        def body(c):
            for hop in range(hops):
                wait_pieces(0, hop, c)
            layer_one(c)

        with jax.named_scope("outer_layer_1"):
            over_chunks(body)
        with jax.named_scope("outer_sent"):
            sent_pieces(1)
        with jax.named_scope("outer_feeds"):
            across[last].open_first()
            for half_block in both_halves:
                across[last].first(half_block).wait_send()
            across[last].relay_own()
            across[last].out.mid(across[last].relay)
            across[last].out.finish(across[last].relay)
        with jax.named_scope("outer_mixed"):
            for which in range(2):
                over_chunks(lambda c: give_mixed(c, which).wait_recv())
        for l in range(split, layers):
            if l < last:
                for half_block in both_halves:
                    across[l].first(half_block).wait_send()
            across[l].out.sent_ring()
            for owner, slot, half_block in across[l].out.blocks():
                across[l].relay(owner, slot, half_block).wait_send()
        sent_pieces(0)

    def open_spare(l):
        if l == last:
            pl.semaphore_wait(r["free"], 3)
        for half_block in both_halves:
            across[l].first(half_block).wait_recv()
        across[l].a.start()

    def relay_spare(l):
        blocks = across[l].b.blocks()
        for owner, slot, half_block in blocks:
            across[l].relay(owner, slot, half_block).wait_recv()
            across[l].mate_b(owner, slot, half_block).start()

    def wait_spare(l):
        across[l].a.wait_mates()
        wait_again(l)

    def wait_again(l):
        for owner, slot, half_block in across[l].b.blocks():
            across[l].mate_b(owner, slot, half_block).wait_recv()

    @pl.when(inner)
    def _():
        with jax.named_scope("forward_0"):
            forward(0, 0, 0, chunks - 1)
        with jax.named_scope("gather_1_mid"):
            gathers[1].mid()
        with jax.named_scope("forward_0b"):
            forward(0, 0, chunks - 1, chunks)
        with jax.named_scope("forward_1"):
            forward(0, 1, 0, 1)
        gathers[split].start()
        with jax.named_scope("forward_1b"):
            forward(0, 1, 1, chunks - 1)
        open_spare(split)
        with jax.named_scope("gather_1_finish"):
            gathers[1].finish()
        with jax.named_scope("forward_1c"):
            forward(0, 1, chunks - 1, chunks)
        with jax.named_scope("gather_1_end"):
            gathers[1].wait_mates()
        with jax.named_scope("layer_1"):
            over_chunks(layer_one)
        with jax.named_scope("gather_2_mid"):
            gathers[split].mid()
        with jax.named_scope("forward_2"):
            forward(1, 0, 0, chunks // 2)
        with jax.named_scope("spare_mid"):
            across[split].a.mid()
        with jax.named_scope("spare_relay"):
            relay_spare(split)
        with jax.named_scope("forward_2b"):
            forward(1, 0, chunks // 2, chunks)
        with jax.named_scope("gather_2_end"):
            gathers[split].finish()
            across[split].a.finish()
        gathers[last].start(2)
        with jax.named_scope("mates_2"):
            gathers[split].wait_mates()
            wait_spare(split)

        def body(c):
            wait_pieces(1, 1, c)
            add_chunk(split, c)
            norm_chunk(split, c)
            branch(split, split, c, place)
            send_piece(split, 0, c)
            branch(split, spare(split), c, end)
            send_piece(split, 1, c)

        with jax.named_scope("layer_2"):
            over_chunks(body, 0, 1)
        with jax.named_scope("spare_open"):
            open_spare(last)
        with jax.named_scope("layer_2b"):
            over_chunks(body, 1, chunks - 1)
        gathers[last].start_ring(2, 4)
        with jax.named_scope("layer_2c"):
            over_chunks(body, chunks - 1, chunks)
        with jax.named_scope("last_spare_mid"):
            across[last].a.mid()
            sent_pieces(1)

        def prepare(c):
            wait_pieces(last - 1, 0, c)
            wait_pieces(last - 1, 1, c)
            add_chunk(last, c)
            norm_chunk(last, c)

        with jax.named_scope("last_norm"):
            over_chunks(prepare, 0, chunks // 2)
        with jax.named_scope("last_mid"):
            gathers[last].mid()
        with jax.named_scope("last_spare"):
            across[last].a.finish()
        with jax.named_scope("last_mates"):
            across[last].a.wait_mates()

        def put_away(c):
            def put(mine, at, value):
                r["b"][1, rows_of(c), mine] = value

            return put

        def put_here(mine, at, value):
            r["mixed"][:, at] = value

        def end_result(which):
            def body(c):
                result(spare(last), rows_of(c), c * part, end, put_away(c), which)
                give_mixed(c, which).start()

            return body

        with jax.named_scope("layer_3_a"):
            over_chunks(end_result(0), 0, chunks // 2)

        def rest(c):
            prepare(c)
            end_result(0)(c)
            end_result(1)(c)

        with jax.named_scope("last_relay"):
            relay_spare(last)
            gathers[last].finish()
            wait_again(last)
        with jax.named_scope("layer_3_b"):
            over_chunks(end_result(1), 0, chunks // 2)
        with jax.named_scope("layer_3_c"):
            over_chunks(rest, chunks // 2, chunks)
        with jax.named_scope("last_gather_end"):
            gathers[last].wait_mates()
        with jax.named_scope("layer_3_own"):
            result(last, pl.ds(0, tok), 0, place, put_here)
        with jax.named_scope("all_sent"):
            sent_pieces(last - 1)
        for l in range(split, layers):
            gathers[l].sent_ring()
            gathers[l].sent_mates()
            across[l].a.sent_ring()
            across[l].a.sent_mates()
            for owner, slot, half_block in across[l].b.blocks():
                across[l].mate_b(owner, slot, half_block).wait_send()
        with jax.named_scope("mixed_sent"):
            for which in range(2):
                over_chunks(lambda c: give_mixed(c, which).wait_send())

    gathers[1].sent_ring()
    gathers[1].sent_mates()


def run_layers(sizes, own, from_last, from_next, tokens, hot, table, gain, counts):
    n_dp, n = sizes
    layers, rows, cols = own.shape
    tok, width = tokens.shape
    chunks = 4
    part = tok // chunks
    half = n_dp // 4
    dma = pltpu.SemaphoreType.DMA
    names = ["own", "from_last", "from_next", "tokens", "hot", "table", "gain", "counts", "mixed"]
    scratch = {
        "w": pltpu.VMEM((layers + 1, n_dp * rows, cols), jnp.bfloat16),
        "stream": pltpu.VMEM((tok, width), jnp.float32),
        "b": pltpu.VMEM((2, tok, width), jnp.bfloat16),
        "x": pltpu.VMEM((tok, width), jnp.bfloat16),
        "own_sem": dma((layers,)),
        "near_sem": dma((2,)),
        "tok_sem": dma((1,)),
        "ring_send": dma((layers + 2, 2, half, 2)),
        "ring_recv": dma((layers + 2, 2, half, 2)),
        "mate_send": dma((layers + 2, 1 + 2 * half, 2)),
        "mate_recv": dma((layers + 2, 1 + 2 * half, 2)),
        "across_send": dma((2, 2 + 2 * half, 2)),
        "across_recv": dma((2, 2 + 2 * half, 2)),
        "again_send": dma((2, 1 + 2 * half, 2)),
        "again_recv": dma((2, 1 + 2 * half, 2)),
        "send": dma((layers - 1, 2, n - 1, chunks)),
        "recv": dma((layers - 1, 2, n - 1, chunks)),
        "mixed_send": dma((2, chunks)),
        "mixed_recv": dma((2, chunks)),
        "free": pltpu.SemaphoreType.REGULAR,
    }
    return pl.pallas_call(
        functools.partial(layers_kernel, n_dp, n, chunks, names + list(scratch)),
        out_shape=jax.ShapeDtypeStruct((tok, cols), jnp.bfloat16),
        in_specs=[ANY, ANY, ANY, ANY, VMEM, VMEM, VMEM, SMEM],
        out_specs=VMEM,
        scratch_shapes=list(scratch.values()),
        compiler_params=pltpu.CompilerParams(
            collective_id=1, has_side_effects=True, vmem_limit_bytes=67043328
        ),
        name="layers",
    )(own, from_last, from_next, tokens, hot, table, gain, counts)


def ring_pairs(n_dp):
    ring = n_dp // 2
    order = [0, 1, 3, 2] if ring == 4 else list(range(ring))
    return [
        (2 * order[i] + core, 2 * order[(i + 1) % ring] + core)
        for i in range(ring)
        for core in range(2)
    ]


def code_table(width):
    quarter = width // 4
    freqs = 1.0 / 10000.0 ** (jnp.arange(quarter, dtype=jnp.float32) / quarter)
    angle = jnp.arange(GRID, dtype=jnp.float32)[:, None] * freqs[None, :]
    exact = jnp.concatenate([jnp.sin(angle), jnp.cos(angle)], axis=1)
    high = lax.reduce_precision(exact, 8, 7)
    middle = lax.reduce_precision(exact - high, 8, 7)
    low = exact - high - middle
    lane = jnp.zeros((GRID, 2 * quarter), jnp.float32)
    return jnp.concatenate([high, middle, low, lane], axis=0).astype(jnp.bfloat16)


def one_hot(patch_index):
    lane = lax.broadcasted_iota(jnp.int32, (1, 1, 4 * GRID), 2)
    which = jnp.stack([patch_index // GRID, patch_index % GRID])[:, :, None]
    return (lane % GRID == which).astype(jnp.bfloat16)


def per_device(
    sizes,
    tokens,
    counts,
    patch_index,
    clip_limit,
    norm_gain,
    params,
    moments,
    seconds,
    gradients,
):
    factor, head = total_over_mesh(sizes, clip_limit, gradients, params, moments, seconds)
    pairs = ring_pairs(sizes[0])
    from_last = lax.ppermute(head, "dp", pairs)
    from_next = lax.ppermute(head, "dp", [(target, source) for source, target in pairs])
    params_new, moments_new, seconds_new, own = adam_all(
        factor, params, moments, seconds, gradients
    )
    table = code_table(tokens.shape[1])
    hot = one_hot(patch_index)
    mixed = run_layers(
        sizes, own, from_last, from_next, tokens, hot, table, norm_gain, counts
    )
    return (params_new, moments_new, seconds_new, mixed)


def solution(mesh):
    sizes = (mesh.shape["dp"], mesh.shape["fsdp"])
    weight = P(None, "dp", "fsdp")
    return jax.shard_map(
        functools.partial(per_device, sizes),
        mesh=mesh,
        in_specs=(P("dp", None), P("dp"), P("dp"), P(), P(), weight, weight, weight, weight),
        out_specs=(weight, weight, weight, P("dp", "fsdp")),
        check_vma=False,
    )
```
